128 devices in a mesh: row: 64 (over z, y, x), col: 2 (over core).
Axes of the slice: x: 4, y: 4, z: 4, core: 2. Of those that a mesh axis runs over, the one named last changes fastest.
Arguments:
- matrix: float32 [12288, 12288], P('row', 'col'), may hold values from -2 to 2, as said below
- diagonal: float32 [12288], P(('row', 'col')), may hold values from 1 to 6
- start: float32 [12288], P(('row', 'col')), may hold values from -6 to 6
Outputs:
- basis: float32 [4, 12288], P(None, ('row', 'col'))
- coefficients: float32 [2, 3], replicated
The draws below stay inside these ranges and needn't reach their ends.
Inputs may be any that keep to these rules, and one draw needn't show every extreme that they name: matrix is exactly symmetric, its entries of order one over the square root of 12288.
All inputs are finite; a program needn't handle non-finite values.
Results may differ from the reference program's by a relative error of at most 0.0003.
Values sent between devices are 32-bit elements.
No kernel may reach another device: no remote copies, remote signals or barrier semaphores. Data moves between devices by JAX's collectives and lax.ppermute only.
A program may use at most 64 MiB of HBM per device.

```python
import math
import jax
import jax.numpy as jnp
from jax import lax

ITERS = 3
DIM = 12288


def draw_matrix(key, part):
    raw_draw = jax.random.normal(key, (DIM, DIM), jnp.float32)
    return (raw_draw + raw_draw.T) * (1.0 / math.sqrt(2.0 * DIM))


def steps_of(key, extent, cuts, low, high):
    def one(position, shards_of):
        heights = jax.random.uniform(jax.random.fold_in(jax.random.fold_in(key, 6), position), (shards_of,), jnp.float32, low / len(cuts), high / len(cuts))
        return jnp.repeat(jnp.exp(heights), extent[position] // shards_of).reshape((-1,) + (1,) * (len(extent) - position - 1))

    level = one(*cuts[0])
    for cut in cuts[1:]:
        level = level * one(*cut)
    return level


def bell_draw(rng, dims, scale, most, cuts=(), dtype=jnp.bfloat16):
    array = scale * jax.random.normal(rng, dims, jnp.float32)
    if cuts:
        array = array * steps_of(rng, dims, cuts, -0.22, 0.18)
    return jnp.clip(array, -most, most).astype(dtype)


def setup_inputs(seed: int = 0) -> dict:
    streams_of = jax.random.split(jax.random.key(seed), 4)
    return {
        "matrix": draw_matrix(jax.random.fold_in(streams_of[3], 71), 0),
        "diagonal": jnp.clip(jnp.exp(math.log(6.0) - 1.7917595 * jax.random.uniform(streams_of[1], (DIM,), jnp.float32) ** steps_of(streams_of[1], (DIM,), ((0, 128),), -0.2, 0.2)), 1.0, 6.0),
        "start": bell_draw(streams_of[2], (DIM,), 1.0, 6.0, ((0, 128),), jnp.float32),
    }


def reference(matrix, diagonal, start):
    full_dim = start.shape[0]
    current = start / jnp.sqrt(jnp.sum(start * start))
    basis_rows = jnp.zeros((ITERS + 1, full_dim), jnp.float32).at[0].set(current)
    alpha_list = []
    beta_list = []
    for iteration in range(ITERS):
        image = jnp.dot(matrix, current, precision=lax.Precision.HIGHEST, preferred_element_type=jnp.float32) + diagonal * current
        intersect = jnp.dot(basis_rows, image, precision=lax.Precision.HIGHEST, preferred_element_type=jnp.float32)
        image = image - jnp.dot(intersect, basis_rows, precision=lax.Precision.HIGHEST, preferred_element_type=jnp.float32)
        beta_value = jnp.sqrt(jnp.sum(image * image))
        current = image / beta_value
        basis_rows = basis_rows.at[iteration + 1].set(current)
        alpha_list.append(intersect[iteration])
        beta_list.append(beta_value)
    coefficients = jnp.stack([jnp.stack(alpha_list), jnp.stack(beta_list)])
    return (basis_rows * jnp.sqrt(jnp.float32(full_dim)), coefficients)
```

```python
import functools
import math

import jax
import jax.numpy as jnp
from jax import lax
from jax.experimental import pallas as pl
from jax.experimental.pallas import tpu as pltpu
from jax.sharding import Mesh
from jax.sharding import PartitionSpec as P

ITERS = 3
LANES = 128
ROW = ("row_0", "row_1", "row_2")
ROW_COL = ("row_0", "row_1", "row_2", "col")


def total(x):
    return jnp.sum(x, axis=(0, 1), keepdims=True)


def lane_of(shape):
    return lax.broadcasted_iota(jnp.int32, shape, 1)


def join_96(parts):
    s0, s1, s2, s3 = parts
    lane = lane_of(s0.shape)
    r1 = pltpu.roll(s1, 96, 1)
    r2 = pltpu.roll(s2, 64, 1)
    r3 = pltpu.roll(s3, 32, 1)
    return jnp.concatenate(
        [jnp.where(lane < 96, s0, r1), jnp.where(lane < 64, r1, r2), jnp.where(lane < 32, r2, r3)], axis=0
    )


def join_192(a0, a1, b0, b1):
    lane = lane_of(a0.shape)
    r0 = pltpu.roll(b0, 64, 1)
    r1 = pltpu.roll(b1, 64, 1)
    return jnp.concatenate([a0, jnp.where(lane < 64, a1, r0), jnp.where(lane < 64, r0, r1)], axis=0)


def gathered_image(g_ref, groups):
    def rows(first):
        return g_ref[pl.ds(first, groups, stride=8), :]

    return join_192(
        rows(0) + rows(2), rows(1) + rows(3), rows(4) + rows(6), rows(5) + rows(7)
    )


def product(vec, scale, m_ref, half_ref, pay_ref):
    groups = vec.shape[0] // 3
    half = groups // 2
    first = lax.axis_index("col") == 0
    for k in range(3):
        lo = vec[k * groups : k * groups + half]
        hi = vec[k * groups + half : (k + 1) * groups]
        half_ref[k * half : (k + 1) * half, :] = jnp.where(first, lo, hi)
    rows = m_ref.shape[0]
    acc = jnp.zeros((rows, LANES), jnp.float32)
    for t in range(m_ref.shape[1] // LANES):
        v = half_ref[pl.ds((t % 3) * half + t // 3, 1), :]
        acc = acc + m_ref[:, t * LANES : (t + 1) * LANES] * v
    top = jnp.sum(acc[:LANES].T, axis=0, keepdims=True)
    low = jnp.concatenate([acc[LANES:], jnp.zeros((2 * LANES - rows, LANES), jnp.float32)], axis=0)
    bottom = jnp.sum(low.T, axis=0, keepdims=True)
    even = lax.broadcasted_iota(jnp.int32, (8, LANES), 0) % 2 == 0
    tile = jnp.where(even, top, bottom) / scale
    for i in range(pay_ref.shape[0] // 8):
        pay_ref[8 * i : 8 * i + 8, :] = tile


def first_kernel(g_ref, m_ref, q_ref, d_ref, pay_ref, half_ref):
    groups = g_ref.shape[0] // 8
    start = join_96([g_ref[pl.ds(2 * j, groups, stride=8), :] for j in range(4)])
    d_ref[...] = join_96([g_ref[pl.ds(2 * j + 1, groups, stride=8), :] for j in range(4)])
    norm = jnp.sqrt(total(start * start))
    q_ref[...] = start / norm
    product(start, norm, m_ref, half_ref, pay_ref)


def orthogonal(g_ref, q_refs, d_ref):
    groups = g_ref.shape[0] // 8
    image = gathered_image(g_ref, groups) + d_ref[...] * q_refs[-1][...]
    dots = [total(q[...] * image) for q in q_refs]
    for h, q in zip(dots, q_refs):
        image = image - h * q[...]
    return image, dots[-1], jnp.sqrt(total(image * image))


def put(coef, row, col, value):
    shape = coef.shape
    at = (lax.broadcasted_iota(jnp.int32, shape, 0) == row) & (lane_of(shape) == col)
    return jnp.where(at, value, coef)


def middle_kernel(k, *refs):
    q_refs = refs[: k + 1]
    d_ref, g_ref, c_ref, m_ref, next_ref, c_out, pay_ref, half_ref = refs[k + 1 :]
    image, alpha, beta = orthogonal(g_ref, q_refs, d_ref)
    next_ref[...] = image / beta
    c_out[...] = put(put(c_ref[...], 0, k, alpha), 1, k, beta)
    product(image, beta, m_ref, half_ref, pay_ref)


def last_kernel(k, full_dim, *refs):
    q_refs = refs[: k + 1]
    d_ref, g_ref, c_ref, basis_ref, c_out, last_ref, piece_ref = refs[k + 1 :]
    image, alpha, beta = orthogonal(g_ref, q_refs, d_ref)
    last_ref[...] = image / beta
    coef = put(put(c_ref[...], 0, k, alpha), 1, k, beta)
    c_out[...] = coef[: c_out.shape[0], : c_out.shape[1]]
    groups = image.shape[0] // 3
    index = lax.axis_index(ROW_COL)
    group = index // 4
    place = index % 4
    for j in range(3):
        for v, q in enumerate((*q_refs, last_ref)):
            piece_ref[8 * j + v : 8 * j + v + 1, :] = q[pl.ds(j * groups + group, 1), :]
    a, b, c = piece_ref[0:8, :], piece_ref[8:16, :], piece_ref[16:24, :]
    lane = lane_of(a.shape)
    one = jnp.where(lane < 32, pltpu.roll(a, 32, 1), pltpu.roll(b, 32, 1))
    two = jnp.where(lane < 64, pltpu.roll(b, 64, 1), pltpu.roll(c, 64, 1))
    three = pltpu.roll(c, 96, 1)
    out = jnp.where(place == 0, a, jnp.where(place == 1, one, jnp.where(place == 2, two, three)))
    out = out * jnp.float32(math.sqrt(full_dim))
    basis_ref[...] = out[: basis_ref.shape[0], : basis_ref.shape[1]]


def call(body, outs, scratch, *args):
    vmem = pl.BlockSpec(memory_space=pltpu.VMEM)
    return pl.pallas_call(
        body,
        out_shape=[jax.ShapeDtypeStruct(s, jnp.float32) for s in outs],
        in_specs=[vmem] * len(args),
        out_specs=[vmem] * len(outs),
        scratch_shapes=[pltpu.VMEM(s, jnp.float32) for s in scratch],
        compiler_params=pltpu.CompilerParams(vmem_limit_bytes=16 << 20),
    )(*args)


def exchange(payload):
    return lax.all_to_all(payload, ROW_COL, 0, 0, tiled=True)


def local(matrix, diagonal, start):
    devices = lax.axis_size(ROW_COL)
    tile_len = start.shape[0]
    full_dim = tile_len * devices
    dense = (full_dim // LANES, LANES)
    half = (full_dim // LANES // 2, LANES)
    pay = (2 * devices, LANES)
    pair = jnp.pad(jnp.stack([start, diagonal]), ((0, 0), (0, LANES - tile_len)))
    gathered = exchange(jnp.broadcast_to(pair[None], (devices, 2, LANES)).reshape(pay))
    q, diag, payload = call(first_kernel, [dense, dense, pay], [half], gathered, matrix)
    basis = [q]
    coef = jnp.zeros((8, LANES), jnp.float32)
    for k in range(ITERS - 1):
        gathered = exchange(payload)
        q, coef, payload = call(
            functools.partial(middle_kernel, k),
            [dense, (8, LANES), pay],
            [half],
            *basis,
            diag,
            gathered,
            coef,
            matrix,
        )
        basis.append(q)
    gathered = exchange(payload)
    return tuple(
        call(
            functools.partial(last_kernel, ITERS - 1, full_dim),
            [(ITERS + 1, tile_len), (2, ITERS)],
            [dense, (24, LANES)],
            *basis,
            diag,
            gathered,
            coef,
        )
    )


def solution(mesh):
    split = Mesh(
        mesh.devices.reshape(4, 4, 4, mesh.shape["col"]), ("row_0", "row_1", "row_2", "col")
    )
    return jax.shard_map(
        local,
        mesh=split,
        in_specs=(P(ROW, "col"), P(ROW_COL), P(ROW_COL)),
        out_specs=(P(None, ROW_COL), P()),
        check_vma=False,
    )
```

```python
import functools
import math

import jax
import jax.numpy as jnp
from jax import lax
from jax.experimental import pallas as pl
from jax.experimental.pallas import tpu as pltpu
from jax.sharding import Mesh
from jax.sharding import PartitionSpec as P

ITERS = 3
LANES = 128
ROW = ("row_0", "row_1", "row_2")
ROW_COL = ("row_0", "row_1", "row_2", "col")


def total(x):
    return jnp.sum(x, axis=(0, 1), keepdims=True)


def lane_of(shape):
    return lax.broadcasted_iota(jnp.int32, shape, 1)


def join_96(parts):
    s0, s1, s2, s3 = parts
    lane = lane_of(s0.shape)
    r1 = pltpu.roll(s1, 96, 1)
    r2 = pltpu.roll(s2, 64, 1)
    r3 = pltpu.roll(s3, 32, 1)
    return jnp.concatenate(
        [jnp.where(lane < 96, s0, r1), jnp.where(lane < 64, r1, r2), jnp.where(lane < 32, r2, r3)], axis=0
    )


def join_192(a0, a1, b0, b1):
    lane = lane_of(a0.shape)
    r0 = pltpu.roll(b0, 64, 1)
    r1 = pltpu.roll(b1, 64, 1)
    return jnp.concatenate([a0, jnp.where(lane < 64, a1, r0), jnp.where(lane < 64, r0, r1)], axis=0)


def gathered_image(g_ref, groups):
    def rows(first):
        return g_ref[pl.ds(first, groups, stride=8), :]

    return join_192(
        rows(0) + rows(2), rows(1) + rows(3), rows(4) + rows(6), rows(5) + rows(7)
    )


def product(vec, scale, m_ref, half_ref, pay_ref):
    groups = vec.shape[0] // 3
    half = groups // 2
    first = lax.axis_index("col") == 0
    for k in range(3):
        lo = vec[k * groups : k * groups + half]
        hi = vec[k * groups + half : (k + 1) * groups]
        half_ref[k * half : (k + 1) * half, :] = jnp.where(first, lo, hi)
    rows = m_ref.shape[0]
    acc = jnp.zeros((rows, LANES), jnp.float32)
    for t in range(m_ref.shape[1] // LANES):
        v = half_ref[pl.ds((t % 3) * half + t // 3, 1), :]
        acc = acc + m_ref[:, t * LANES : (t + 1) * LANES] * v
    top = jnp.sum(acc[:LANES].T, axis=0, keepdims=True)
    low = jnp.concatenate([acc[LANES:], jnp.zeros((2 * LANES - rows, LANES), jnp.float32)], axis=0)
    bottom = jnp.sum(low.T, axis=0, keepdims=True)
    even = lax.broadcasted_iota(jnp.int32, (8, LANES), 0) % 2 == 0
    tile = jnp.where(even, top, bottom) / scale
    for i in range(pay_ref.shape[0] // 8):
        pay_ref[8 * i : 8 * i + 8, :] = tile


def pair_kernel(s_ref, d_ref, _, pay_ref, s_got, d_got, pair_ref, sems):
    copies = [
        pltpu.make_async_copy(s_ref, s_got, sems.at[0]),
        pltpu.make_async_copy(d_ref, d_got, sems.at[1]),
    ]
    for copy in copies:
        copy.start()
    pair_ref[...] = jnp.zeros(pair_ref.shape, jnp.float32)
    for copy in copies:
        copy.wait()
    width = s_got.shape[1]
    pair_ref[0:1, 0:width] = s_got[...]
    pair_ref[1:2, 0:width] = d_got[...]
    even = lax.broadcasted_iota(jnp.int32, (8, LANES), 0) % 2 == 0
    tile = jnp.where(even, pair_ref[0:1, :], pair_ref[1:2, :])
    for i in range(pay_ref.shape[0] // 8):
        pay_ref[8 * i : 8 * i + 8, :] = tile


def first_kernel(g_ref, m_ref, q_ref, d_ref, pay_ref, half_ref):
    groups = g_ref.shape[0] // 8
    start = join_96([g_ref[pl.ds(2 * j, groups, stride=8), :] for j in range(4)])
    d_ref[...] = join_96([g_ref[pl.ds(2 * j + 1, groups, stride=8), :] for j in range(4)])
    norm = jnp.sqrt(total(start * start))
    q_ref[...] = start / norm
    product(start, norm, m_ref, half_ref, pay_ref)


def orthogonal(g_ref, q_refs, d_ref):
    groups = g_ref.shape[0] // 8
    image = gathered_image(g_ref, groups) + d_ref[...] * q_refs[-1][...]
    dots = [total(q[...] * image) for q in q_refs]
    for h, q in zip(dots, q_refs):
        image = image - h * q[...]
    return image, dots[-1], jnp.sqrt(total(image * image))


def put(coef, row, col, value):
    shape = coef.shape
    at = (lax.broadcasted_iota(jnp.int32, shape, 0) == row) & (lane_of(shape) == col)
    return jnp.where(at, value, coef)


def middle_kernel(k, *refs):
    q_refs = refs[: k + 1]
    d_ref, g_ref, c_ref, m_ref, next_ref, c_out, pay_ref, half_ref = refs[k + 1 :]
    image, alpha, beta = orthogonal(g_ref, q_refs, d_ref)
    next_ref[...] = image / beta
    c_out[...] = put(put(c_ref[...], 0, k, alpha), 1, k, beta)
    product(image, beta, m_ref, half_ref, pay_ref)


def last_kernel(k, full_dim, *refs):
    q_refs = refs[: k + 1]
    d_ref, g_ref, c_ref, basis_ref, c_out, last_ref, piece_ref = refs[k + 1 :]
    image, alpha, beta = orthogonal(g_ref, q_refs, d_ref)
    last_ref[...] = image / beta
    coef = put(put(c_ref[...], 0, k, alpha), 1, k, beta)
    c_out[...] = coef[: c_out.shape[0], : c_out.shape[1]]
    groups = image.shape[0] // 3
    index = lax.axis_index(ROW_COL)
    group = index // 4
    place = index % 4
    for j in range(3):
        for v, q in enumerate((*q_refs, last_ref)):
            piece_ref[8 * j + v : 8 * j + v + 1, :] = q[pl.ds(j * groups + group, 1), :]
    a, b, c = piece_ref[0:8, :], piece_ref[8:16, :], piece_ref[16:24, :]
    lane = lane_of(a.shape)
    one = jnp.where(lane < 32, pltpu.roll(a, 32, 1), pltpu.roll(b, 32, 1))
    two = jnp.where(lane < 64, pltpu.roll(b, 64, 1), pltpu.roll(c, 64, 1))
    three = pltpu.roll(c, 96, 1)
    out = jnp.where(place == 0, a, jnp.where(place == 1, one, jnp.where(place == 2, two, three)))
    out = out * jnp.float32(math.sqrt(full_dim))
    basis_ref[...] = out[: basis_ref.shape[0], : basis_ref.shape[1]]


def call(body, outs, scratch, *args):
    vmem = pl.BlockSpec(memory_space=pltpu.VMEM)
    return pl.pallas_call(
        body,
        out_shape=[jax.ShapeDtypeStruct(s, jnp.float32) for s in outs],
        in_specs=[vmem] * len(args),
        out_specs=[vmem] * len(outs),
        scratch_shapes=[pltpu.VMEM(s, jnp.float32) for s in scratch],
        compiler_params=pltpu.CompilerParams(vmem_limit_bytes=16 << 20),
    )(*args)


def pair_call(pay, start, diagonal, matrix):
    hbm = pl.BlockSpec(memory_space=pltpu.HBM)
    cost = pl.CostEstimate(flops=0, transcendentals=0, bytes_accessed=4 * matrix.nbytes)
    return pl.pallas_call(
        pair_kernel,
        out_shape=jax.ShapeDtypeStruct(pay, jnp.float32),
        in_specs=[hbm] * 3,
        out_specs=pl.BlockSpec(memory_space=pltpu.VMEM),
        scratch_shapes=[
            pltpu.VMEM(start.shape, jnp.float32),
            pltpu.VMEM(diagonal.shape, jnp.float32),
            pltpu.VMEM((8, LANES), jnp.float32),
            pltpu.SemaphoreType.DMA((2,)),
        ],
        cost_estimate=cost,
        compiler_params=pltpu.CompilerParams(vmem_limit_bytes=16 << 20),
    )(*(pltpu.with_memory_space_constraint(x, pltpu.HBM) for x in (start, diagonal, matrix)))


def exchange(payload):
    return lax.all_to_all(payload, ROW_COL, 0, 0, tiled=True)


def local(matrix, diagonal, start):
    devices = lax.axis_size(ROW_COL)
    tile_len = start.shape[0]
    full_dim = tile_len * devices
    dense = (full_dim // LANES, LANES)
    half = (full_dim // LANES // 2, LANES)
    pay = (2 * devices, LANES)
    payload = pair_call(pay, start.reshape(1, -1), diagonal.reshape(1, -1), matrix)
    gathered = exchange(payload)
    q, diag, payload = call(first_kernel, [dense, dense, pay], [half], gathered, matrix)
    basis = [q]
    coef = jnp.zeros((8, LANES), jnp.float32)
    for k in range(ITERS - 1):
        gathered = exchange(payload)
        q, coef, payload = call(
            functools.partial(middle_kernel, k),
            [dense, (8, LANES), pay],
            [half],
            *basis,
            diag,
            gathered,
            coef,
            matrix,
        )
        basis.append(q)
    gathered = exchange(payload)
    return tuple(
        call(
            functools.partial(last_kernel, ITERS - 1, full_dim),
            [(ITERS + 1, tile_len), (2, ITERS)],
            [dense, (24, LANES)],
            *basis,
            diag,
            gathered,
            coef,
        )
    )


def solution(mesh):
    split = Mesh(
        mesh.devices.reshape(4, 4, 4, mesh.shape["col"]), ("row_0", "row_1", "row_2", "col")
    )
    return jax.shard_map(
        local,
        mesh=split,
        in_specs=(P(ROW, "col"), P(ROW_COL), P(ROW_COL)),
        out_specs=(P(None, ROW_COL), P()),
        check_vma=False,
    )
```

```python
import functools
import math

import jax
import jax.numpy as jnp
from jax import lax
from jax.experimental import pallas as pl
from jax.experimental.pallas import tpu as pltpu
from jax.sharding import Mesh
from jax.sharding import PartitionSpec as P

ITERS = 3
LANES = 128
ROW = ("row_0", "row_1", "row_2")
ROW_COL = ("row_0", "row_1", "row_2", "col")
ORDER = ("col", "row_2", "row_1", "row_0")
SIDE = 4
PLANE = SIDE * SIDE


def total(x):
    return jnp.sum(x, axis=(0, 1), keepdims=True)


def lane_of(shape):
    return lax.broadcasted_iota(jnp.int32, shape, 1)


def join_96(parts):
    s0, s1, s2, s3 = parts
    lane = lane_of(s0.shape)
    r1 = pltpu.roll(s1, 96, 1)
    r2 = pltpu.roll(s2, 64, 1)
    r3 = pltpu.roll(s3, 32, 1)
    return jnp.concatenate(
        [jnp.where(lane < 96, s0, r1), jnp.where(lane < 64, r1, r2), jnp.where(lane < 32, r2, r3)], axis=0
    )


def join_192(a0, a1, b0, b1):
    lane = lane_of(a0.shape)
    r0 = pltpu.roll(b0, 64, 1)
    r1 = pltpu.roll(b1, 64, 1)
    return jnp.concatenate([a0, jnp.where(lane < 64, a1, r0), jnp.where(lane < 64, r0, r1)], axis=0)


def rows_of(g_ref, col, parity, part):
    devices = g_ref.shape[0] // 2
    return jnp.concatenate(
        [
            g_ref[pl.ds(col * devices + 2 * PLANE * (2 * u + parity) + part, PLANE, stride=2), :]
            for u in range(SIDE // 2)
        ],
        axis=0,
    )


def gathered_image(g_ref):
    a0, a1, b0, b1 = (
        rows_of(g_ref, 0, parity, part) + rows_of(g_ref, 1, parity, part)
        for parity in range(2)
        for part in range(2)
    )
    return join_192(a0, a1, b0, b1)


def product(vec, m_ref, vec_ref):
    vec_ref[...] = vec
    groups = vec.shape[0] // 3
    shift = lax.axis_index("col") * (SIDE // 2)
    rows = m_ref.shape[0]
    acc = jnp.zeros((rows, LANES), jnp.float32)
    for t in range(m_ref.shape[1] // LANES):
        group, k = t // 3, t % 3
        z, y, u = group // (2 * SIDE), group // 2 % SIDE, group % 2
        v = vec_ref[pl.ds(shift + (k * groups + u * PLANE + y * SIDE + z), 1), :]
        acc = acc + m_ref[:, t * LANES : (t + 1) * LANES] * v
    top = jnp.sum(acc[:LANES].T, axis=0, keepdims=True)
    low = jnp.concatenate([acc[LANES:], jnp.zeros((2 * LANES - rows, LANES), jnp.float32)], axis=0)
    bottom = jnp.sum(low.T, axis=0, keepdims=True)
    even = lax.broadcasted_iota(jnp.int32, (8, LANES), 0) % 2 == 0
    return jnp.where(even, top, bottom)


def fill(pay_ref, tile):
    for i in range(pay_ref.shape[0] // 8):
        pay_ref[8 * i : 8 * i + 8, :] = tile


def pair_kernel(s_ref, d_ref, _, pay_ref, s_got, d_got, pair_ref, sems):
    copies = [
        pltpu.make_async_copy(s_ref, s_got, sems.at[0]),
        pltpu.make_async_copy(d_ref, d_got, sems.at[1]),
    ]
    for copy in copies:
        copy.start()
    pair_ref[...] = jnp.zeros(pair_ref.shape, jnp.float32)
    for copy in copies:
        copy.wait()
    width = s_got.shape[1]
    pair_ref[0:1, 0:width] = s_got[...]
    pair_ref[1:2, 0:width] = d_got[...]
    even = lax.broadcasted_iota(jnp.int32, (8, LANES), 0) % 2 == 0
    fill(pay_ref, jnp.where(even, pair_ref[0:1, :], pair_ref[1:2, :]))


def first_kernel(g_ref, m_ref, q_ref, d_ref, tile_ref, pay_ref, vec_ref):
    start, diag = (
        join_96([rows_of(g_ref, j % 2, j // 2, part) for j in range(4)]) for part in range(2)
    )
    d_ref[...] = diag
    tile = product(start, m_ref, vec_ref)
    scale = 1.0 / jnp.sqrt(total(start * start))
    q_ref[...] = start * scale
    tile = tile * scale
    tile_ref[...] = tile
    fill(pay_ref, tile)


def orthogonal(image, q_refs):
    dots = [total(q[...] * image) for q in q_refs]
    for h, q in zip(dots, q_refs):
        image = image - h * q[...]
    return image, dots, jnp.sqrt(total(image * image))


def put(coef, row, col, value):
    shape = coef.shape
    at = (lax.broadcasted_iota(jnp.int32, shape, 0) == row) & (lane_of(shape) == col)
    return jnp.where(at, value, coef)


def middle_kernel(k, *refs):
    q_refs, tile_refs = refs[: k + 1], refs[k + 1 : 2 * k + 2]
    d_ref, g_ref, c_ref, m_ref, next_ref, c_out, tile_ref, pay_ref, vec_ref = refs[2 * k + 2 :]
    image = gathered_image(g_ref) + d_ref[...] * q_refs[-1][...]
    tile = product(image, m_ref, vec_ref)
    image, dots, beta = orthogonal(image, q_refs)
    scale = 1.0 / beta
    next_ref[...] = image * scale
    c_out[...] = put(put(c_ref[...], 0, k, dots[-1]), 1, k, beta)
    for h, t in zip(dots, tile_refs):
        tile = tile - h * t[...]
    tile = tile * scale
    tile_ref[...] = tile
    fill(pay_ref, tile)


def last_kernel(k, full_dim, *refs):
    q_refs = refs[: k + 1]
    d_ref, g_ref, c_ref, basis_ref, c_out, last_ref, piece_ref = refs[k + 1 :]
    image = gathered_image(g_ref) + d_ref[...] * q_refs[-1][...]
    image, dots, beta = orthogonal(image, q_refs)
    alpha = dots[-1]
    last_ref[...] = image * (1.0 / beta)
    coef = put(put(c_ref[...], 0, k, alpha), 1, k, beta)
    c_out[...] = coef[: c_out.shape[0], : c_out.shape[1]]
    groups = image.shape[0] // 3
    x = lax.axis_index("row_2")
    group = x // 2 * PLANE + lax.axis_index("row_1") * SIDE + lax.axis_index("row_0")
    place = x % 2 * 2 + lax.axis_index("col")
    for j in range(3):
        for v, q in enumerate((*q_refs, last_ref)):
            piece_ref[8 * j + v : 8 * j + v + 1, :] = q[pl.ds(j * groups + group, 1), :]
    a, b, c = piece_ref[0:8, :], piece_ref[8:16, :], piece_ref[16:24, :]
    lane = lane_of(a.shape)
    one = jnp.where(lane < 32, pltpu.roll(a, 32, 1), pltpu.roll(b, 32, 1))
    two = jnp.where(lane < 64, pltpu.roll(b, 64, 1), pltpu.roll(c, 64, 1))
    three = pltpu.roll(c, 96, 1)
    out = jnp.where(place == 0, a, jnp.where(place == 1, one, jnp.where(place == 2, two, three)))
    out = out * jnp.float32(math.sqrt(full_dim))
    basis_ref[...] = out[: basis_ref.shape[0], : basis_ref.shape[1]]


def call(body, outs, scratch, *args):
    vmem = pl.BlockSpec(memory_space=pltpu.VMEM)
    return pl.pallas_call(
        body,
        out_shape=[jax.ShapeDtypeStruct(s, jnp.float32) for s in outs],
        in_specs=[vmem] * len(args),
        out_specs=[vmem] * len(outs),
        scratch_shapes=[pltpu.VMEM(s, jnp.float32) for s in scratch],
        compiler_params=pltpu.CompilerParams(vmem_limit_bytes=16 << 20),
    )(*args)


def pair_call(pay, start, diagonal, matrix):
    hbm = pl.BlockSpec(memory_space=pltpu.HBM)
    cost = pl.CostEstimate(flops=0, transcendentals=0, bytes_accessed=4 * matrix.nbytes)
    return pl.pallas_call(
        pair_kernel,
        out_shape=jax.ShapeDtypeStruct(pay, jnp.float32),
        in_specs=[hbm] * 3,
        out_specs=pl.BlockSpec(memory_space=pltpu.VMEM),
        scratch_shapes=[
            pltpu.VMEM(start.shape, jnp.float32),
            pltpu.VMEM(diagonal.shape, jnp.float32),
            pltpu.VMEM((8, LANES), jnp.float32),
            pltpu.SemaphoreType.DMA((2,)),
        ],
        cost_estimate=cost,
        compiler_params=pltpu.CompilerParams(vmem_limit_bytes=16 << 20),
    )(*(pltpu.with_memory_space_constraint(x, pltpu.HBM) for x in (start, diagonal, matrix)))


def exchange(payload):
    return lax.all_to_all(payload, ORDER, 0, 0, tiled=True)


def local(matrix, diagonal, start):
    devices = lax.axis_size(ROW_COL)
    tile_len = start.shape[0]
    full_dim = tile_len * devices
    dense = (full_dim // LANES, LANES)
    pay = (2 * devices, LANES)
    payload = pair_call(pay, start.reshape(1, -1), diagonal.reshape(1, -1), matrix)
    gathered = exchange(payload)
    tile = (8, LANES)
    q, diag, part, payload = call(first_kernel, [dense, dense, tile, pay], [dense], gathered, matrix)
    basis, parts = [q], [part]
    coef = jnp.zeros(tile, jnp.float32)
    for k in range(ITERS - 1):
        gathered = exchange(payload)
        q, coef, part, payload = call(
            functools.partial(middle_kernel, k),
            [dense, tile, tile, pay],
            [dense],
            *basis,
            *parts,
            diag,
            gathered,
            coef,
            matrix,
        )
        basis.append(q)
        parts.append(part)
    gathered = exchange(payload)
    return tuple(
        call(
            functools.partial(last_kernel, ITERS - 1, full_dim),
            [(ITERS + 1, tile_len), (2, ITERS)],
            [dense, (24, LANES)],
            *basis,
            diag,
            gathered,
            coef,
        )
    )


def solution(mesh):
    split = Mesh(
        mesh.devices.reshape(4, 4, 4, mesh.shape["col"]), ("row_0", "row_1", "row_2", "col")
    )
    return jax.shard_map(
        local,
        mesh=split,
        in_specs=(P(ROW, "col"), P(ROW_COL), P(ROW_COL)),
        out_specs=(P(None, ROW_COL), P()),
        check_vma=False,
    )
```

```python
import functools
import math

import jax
import jax.numpy as jnp
from jax import lax
from jax.experimental import pallas as pl
from jax.experimental.pallas import tpu as pltpu
from jax.sharding import Mesh
from jax.sharding import PartitionSpec as P

ITERS = 3
LANES = 128
ROW = ("row_0", "row_1", "row_2")
ROW_COL = ("row_0", "row_1", "row_2", "col")
ORDER = ("col", "row_2", "row_1", "row_0")
SIDE = 4
PLANE = SIDE * SIDE


def total(x):
    return jnp.sum(x, axis=(0, 1), keepdims=True)


def lane_of(shape):
    return lax.broadcasted_iota(jnp.int32, shape, 1)


def join_96(parts):
    s0, s1, s2, s3 = parts
    lane = lane_of(s0.shape)
    r1 = pltpu.roll(s1, 96, 1)
    r2 = pltpu.roll(s2, 64, 1)
    r3 = pltpu.roll(s3, 32, 1)
    return jnp.concatenate(
        [jnp.where(lane < 96, s0, r1), jnp.where(lane < 64, r1, r2), jnp.where(lane < 32, r2, r3)], axis=0
    )


def join_192(a0, a1, b0, b1):
    lane = lane_of(a0.shape)
    r0 = pltpu.roll(b0, 64, 1)
    r1 = pltpu.roll(b1, 64, 1)
    return jnp.concatenate([a0, jnp.where(lane < 64, a1, r0), jnp.where(lane < 64, r0, r1)], axis=0)


def rows_of(g_ref, col, parity, part):
    devices = g_ref.shape[0] // 2
    return jnp.concatenate(
        [
            g_ref[pl.ds(col * devices + 2 * PLANE * (2 * u + parity) + part, PLANE, stride=2), :]
            for u in range(SIDE // 2)
        ],
        axis=0,
    )


def gathered_image(g_ref):
    a0, a1, b0, b1 = (
        rows_of(g_ref, 0, parity, part) + rows_of(g_ref, 1, parity, part)
        for parity in range(2)
        for part in range(2)
    )
    return join_192(a0, a1, b0, b1)


def product(vec, m_ref, vec_ref):
    if vec is not None:
        vec_ref[...] = vec
    groups = vec_ref.shape[0] // 3
    shift = lax.axis_index("col") * (SIDE // 2)
    rows = m_ref.shape[0]
    acc = jnp.zeros((rows, LANES), jnp.float32)
    for t in range(m_ref.shape[1] // LANES):
        group, k = t // 3, t % 3
        z, y, u = group // (2 * SIDE), group // 2 % SIDE, group % 2
        v = vec_ref[pl.ds(shift + (k * groups + u * PLANE + y * SIDE + z), 1), :]
        acc = acc + m_ref[:, t * LANES : (t + 1) * LANES] * v
    top = jnp.sum(acc[:LANES].T, axis=0, keepdims=True)
    low = jnp.concatenate([acc[LANES:], jnp.zeros((2 * LANES - rows, LANES), jnp.float32)], axis=0)
    bottom = jnp.sum(low.T, axis=0, keepdims=True)
    even = lax.broadcasted_iota(jnp.int32, (8, LANES), 0) % 2 == 0
    return jnp.where(even, top, bottom)


def fill(pay_ref, tile):
    for i in range(pay_ref.shape[0] // 8):
        pay_ref[8 * i : 8 * i + 8, :] = tile


def pair_kernel(s_ref, d_ref, _, pay_ref, s_got, d_got, pair_ref, sems):
    copies = [
        pltpu.make_async_copy(s_ref, s_got, sems.at[0]),
        pltpu.make_async_copy(d_ref, d_got, sems.at[1]),
    ]
    for copy in copies:
        copy.start()
    pair_ref[...] = jnp.zeros(pair_ref.shape, jnp.float32)
    for copy in copies:
        copy.wait()
    width = s_got.shape[1]
    pair_ref[0:1, 0:width] = s_got[...]
    pair_ref[1:2, 0:width] = d_got[...]
    even = lax.broadcasted_iota(jnp.int32, (8, LANES), 0) % 2 == 0
    fill(pay_ref, jnp.where(even, pair_ref[0:1, :], pair_ref[1:2, :]))


def first_kernel(g_ref, m_ref, q_ref, d_ref, tile_ref, pay_ref, vec_ref):
    start, diag = (
        join_96([rows_of(g_ref, j % 2, j // 2, part) for j in range(4)]) for part in range(2)
    )
    d_ref[...] = diag
    tile = product(start, m_ref, vec_ref)
    scale = 1.0 / jnp.sqrt(total(start * start))
    q_ref[...] = start * scale
    tile = tile * scale
    tile_ref[...] = tile
    fill(pay_ref, tile)


def dots_of(image, q_refs):
    return [total(q[...] * image) for q in q_refs]


def orthogonal(image, dots, q_refs):
    for h, q in zip(dots, q_refs):
        image = image - h * q[...]
    return image, jnp.sqrt(total(image * image))


def put(coef, row, col, value):
    shape = coef.shape
    at = (lax.broadcasted_iota(jnp.int32, shape, 0) == row) & (lane_of(shape) == col)
    return jnp.where(at, value, coef)


def middle_kernel(k, *refs):
    q_refs, tile_refs = refs[: k + 1], refs[k + 1 : 2 * k + 2]
    d_ref, g_ref, c_ref, m_ref, next_ref, c_out, pay_ref, *out_refs, vec_ref = refs[2 * k + 2 :]
    image = gathered_image(g_ref) + d_ref[...] * q_refs[-1][...]
    dots = dots_of(image, q_refs)
    vec_ref[...] = image
    image, beta = orthogonal(image, dots, q_refs)
    tile = product(None, m_ref, vec_ref)
    scale = 1.0 / beta
    next_ref[...] = image * scale
    c_out[...] = put(put(c_ref[...], 0, k, dots[-1]), 1, k, beta)
    for h, t in zip(dots, tile_refs):
        tile = tile - h * t[...]
    tile = tile * scale
    for tile_ref in out_refs:
        tile_ref[...] = tile
    fill(pay_ref, tile)


def last_kernel(k, full_dim, *refs):
    q_refs = refs[: k + 1]
    d_ref, g_ref, c_ref, basis_ref, c_out, last_ref, piece_ref = refs[k + 1 :]
    image = gathered_image(g_ref) + d_ref[...] * q_refs[-1][...]
    dots = dots_of(image, q_refs)
    image, beta = orthogonal(image, dots, q_refs)
    last_ref[...] = image
    coef = put(put(c_ref[...], 0, k, dots[-1]), 1, k, beta)
    c_out[...] = coef[: c_out.shape[0], : c_out.shape[1]]
    groups = image.shape[0] // 3
    x = lax.axis_index("row_2")
    group = x // 2 * PLANE + lax.axis_index("row_1") * SIDE + lax.axis_index("row_0")
    place = x % 2 * 2 + lax.axis_index("col")
    for j in range(3):
        for v, q in enumerate((*q_refs, last_ref)):
            piece_ref[8 * j + v : 8 * j + v + 1, :] = q[pl.ds(j * groups + group, 1), :]
    a, b, c = piece_ref[0:8, :], piece_ref[8:16, :], piece_ref[16:24, :]
    lane = lane_of(a.shape)
    one = jnp.where(lane < 32, pltpu.roll(a, 32, 1), pltpu.roll(b, 32, 1))
    two = jnp.where(lane < 64, pltpu.roll(b, 64, 1), pltpu.roll(c, 64, 1))
    three = pltpu.roll(c, 96, 1)
    out = jnp.where(place == 0, a, jnp.where(place == 1, one, jnp.where(place == 2, two, three)))
    newest = lax.broadcasted_iota(jnp.int32, out.shape, 0) == len(q_refs)
    out = out * jnp.float32(math.sqrt(full_dim)) * jnp.where(newest, 1.0 / beta, 1.0)
    basis_ref[...] = out[: basis_ref.shape[0], : basis_ref.shape[1]]


def call(body, outs, scratch, *args):
    vmem = pl.BlockSpec(memory_space=pltpu.VMEM)
    return pl.pallas_call(
        body,
        out_shape=[jax.ShapeDtypeStruct(s, jnp.float32) for s in outs],
        in_specs=[vmem] * len(args),
        out_specs=[vmem] * len(outs),
        scratch_shapes=[pltpu.VMEM(s, jnp.float32) for s in scratch],
        compiler_params=pltpu.CompilerParams(vmem_limit_bytes=16 << 20),
    )(*args)


def pair_call(pay, start, diagonal, matrix):
    hbm = pl.BlockSpec(memory_space=pltpu.HBM)
    cost = pl.CostEstimate(flops=0, transcendentals=0, bytes_accessed=4 * matrix.nbytes)
    return pl.pallas_call(
        pair_kernel,
        out_shape=jax.ShapeDtypeStruct(pay, jnp.float32),
        in_specs=[hbm] * 3,
        out_specs=pl.BlockSpec(memory_space=pltpu.VMEM),
        scratch_shapes=[
            pltpu.VMEM(start.shape, jnp.float32),
            pltpu.VMEM(diagonal.shape, jnp.float32),
            pltpu.VMEM((8, LANES), jnp.float32),
            pltpu.SemaphoreType.DMA((2,)),
        ],
        cost_estimate=cost,
        compiler_params=pltpu.CompilerParams(vmem_limit_bytes=16 << 20),
    )(*(pltpu.with_memory_space_constraint(x, pltpu.HBM) for x in (start, diagonal, matrix)))


def exchange(payload):
    return lax.all_to_all(payload, ORDER, 0, 0, tiled=True)


def local(matrix, diagonal, start):
    devices = lax.axis_size(ROW_COL)
    tile_len = start.shape[0]
    full_dim = tile_len * devices
    dense = (full_dim // LANES, LANES)
    pay = (2 * devices, LANES)
    payload = pair_call(pay, start.reshape(1, -1), diagonal.reshape(1, -1), matrix)
    gathered = exchange(payload)
    tile = (8, LANES)
    q, diag, part, payload = call(first_kernel, [dense, dense, tile, pay], [dense], gathered, matrix)
    basis, parts = [q], [part]
    coef = jnp.zeros(tile, jnp.float32)
    for k in range(ITERS - 1):
        gathered = exchange(payload)
        q, coef, payload, *part = call(
            functools.partial(middle_kernel, k),
            [dense, tile, pay] + [tile] * (k < ITERS - 2),
            [dense],
            *basis,
            *parts,
            diag,
            gathered,
            coef,
            matrix,
        )
        basis.append(q)
        parts += part
    gathered = exchange(payload)
    return tuple(
        call(
            functools.partial(last_kernel, ITERS - 1, full_dim),
            [(ITERS + 1, tile_len), (2, ITERS)],
            [dense, (24, LANES)],
            *basis,
            diag,
            gathered,
            coef,
        )
    )


def solution(mesh):
    split = Mesh(
        mesh.devices.reshape(4, 4, 4, mesh.shape["col"]), ("row_0", "row_1", "row_2", "col")
    )
    return jax.shard_map(
        local,
        mesh=split,
        in_specs=(P(ROW, "col"), P(ROW_COL), P(ROW_COL)),
        out_specs=(P(None, ROW_COL), P()),
        check_vma=False,
    )
```

```python
import functools
import math

import jax
import jax.numpy as jnp
from jax import lax
from jax.experimental import pallas as pl
from jax.experimental.pallas import tpu as pltpu
from jax.sharding import Mesh
from jax.sharding import PartitionSpec as P

ITERS = 3
LANES = 128
ROW = ("row_0", "row_1", "row_2")
ROW_COL = ("row_0", "row_1", "row_2", "col")
ORDER = ("col", "row_0", "row_1", "row_2")


def total(x):
    return jnp.sum(x, axis=(0, 1), keepdims=True)


def lane_of(shape):
    return lax.broadcasted_iota(jnp.int32, shape, 1)


def join_96(parts):
    s0, s1, s2, s3 = parts
    lane = lane_of(s0.shape)
    r1 = pltpu.roll(s1, 96, 1)
    r2 = pltpu.roll(s2, 64, 1)
    r3 = pltpu.roll(s3, 32, 1)
    return jnp.concatenate(
        [jnp.where(lane < 96, s0, r1), jnp.where(lane < 64, r1, r2), jnp.where(lane < 32, r2, r3)], axis=0
    )


def join_192(a0, a1, b0, b1):
    lane = lane_of(a0.shape)
    r0 = pltpu.roll(b0, 64, 1)
    r1 = pltpu.roll(b1, 64, 1)
    return jnp.concatenate([a0, jnp.where(lane < 64, a1, r0), jnp.where(lane < 64, r0, r1)], axis=0)


def rows_of(g_ref, col, parity, part):
    devices = g_ref.shape[0] // 2
    return g_ref[pl.ds(col * devices + 2 * parity + part, devices // 4, stride=4), :]


def gathered_image(g_ref):
    a0, a1, b0, b1 = (
        rows_of(g_ref, 0, parity, part) + rows_of(g_ref, 1, parity, part)
        for parity in range(2)
        for part in range(2)
    )
    return join_192(a0, a1, b0, b1)


def product(vec, m_ref, vec_ref):
    if vec is not None:
        vec_ref[...] = vec
    groups = vec_ref.shape[0] // 3
    shift = lax.axis_index("col") * (groups // 2)
    rows = m_ref.shape[0]
    acc = jnp.zeros((rows, LANES), jnp.float32)
    for t in range(m_ref.shape[1] // LANES):
        v = vec_ref[pl.ds(shift + (t % 3 * groups + t // 3), 1), :]
        acc = acc + m_ref[:, t * LANES : (t + 1) * LANES] * v
    top = jnp.sum(acc[:LANES].T, axis=0, keepdims=True)
    low = jnp.concatenate([acc[LANES:], jnp.zeros((2 * LANES - rows, LANES), jnp.float32)], axis=0)
    bottom = jnp.sum(low.T, axis=0, keepdims=True)
    even = lax.broadcasted_iota(jnp.int32, (8, LANES), 0) % 2 == 0
    return jnp.where(even, top, bottom)


def fill(pay_ref, tile):
    for i in range(pay_ref.shape[0] // 8):
        pay_ref[8 * i : 8 * i + 8, :] = tile


def pair_kernel(s_ref, d_ref, _, pay_ref, s_got, d_got, pair_ref, sems):
    copies = [
        pltpu.make_async_copy(s_ref, s_got, sems.at[0]),
        pltpu.make_async_copy(d_ref, d_got, sems.at[1]),
    ]
    for copy in copies:
        copy.start()
    pair_ref[...] = jnp.zeros(pair_ref.shape, jnp.float32)
    for copy in copies:
        copy.wait()
    width = s_got.shape[1]
    pair_ref[0:1, 0:width] = s_got[...]
    pair_ref[1:2, 0:width] = d_got[...]
    even = lax.broadcasted_iota(jnp.int32, (8, LANES), 0) % 2 == 0
    fill(pay_ref, jnp.where(even, pair_ref[0:1, :], pair_ref[1:2, :]))


def first_kernel(g_ref, m_ref, q_ref, d_ref, tile_ref, pay_ref, vec_ref):
    start, diag = (
        join_96([rows_of(g_ref, j % 2, j // 2, part) for j in range(4)]) for part in range(2)
    )
    d_ref[...] = diag
    tile = product(start, m_ref, vec_ref)
    scale = 1.0 / jnp.sqrt(total(start * start))
    q_ref[...] = start * scale
    tile = tile * scale
    tile_ref[...] = tile
    fill(pay_ref, tile)


def dots_of(image, q_refs):
    return [total(q[...] * image) for q in q_refs]


def orthogonal(image, dots, q_refs):
    for h, q in zip(dots, q_refs):
        image = image - h * q[...]
    return image, jnp.sqrt(total(image * image))


def put(coef, row, col, value):
    shape = coef.shape
    at = (lax.broadcasted_iota(jnp.int32, shape, 0) == row) & (lane_of(shape) == col)
    return jnp.where(at, value, coef)


def middle_kernel(k, *refs):
    q_refs, tile_refs = refs[: k + 1], refs[k + 1 : 2 * k + 2]
    d_ref, g_ref, c_ref, m_ref, next_ref, c_out, pay_ref, *out_refs, vec_ref = refs[2 * k + 2 :]
    image = gathered_image(g_ref) + d_ref[...] * q_refs[-1][...]
    dots = dots_of(image, q_refs)
    vec_ref[...] = image
    image, beta = orthogonal(image, dots, q_refs)
    tile = product(None, m_ref, vec_ref)
    scale = 1.0 / beta
    next_ref[...] = image * scale
    c_out[...] = put(put(c_ref[...], 0, k, dots[-1]), 1, k, beta)
    for h, t in zip(dots, tile_refs):
        tile = tile - h * t[...]
    tile = tile * scale
    for tile_ref in out_refs:
        tile_ref[...] = tile
    fill(pay_ref, tile)


def last_kernel(k, full_dim, *refs):
    q_refs = refs[: k + 1]
    d_ref, g_ref, c_ref, basis_ref, c_out, last_ref, piece_ref = refs[k + 1 :]
    image = gathered_image(g_ref) + d_ref[...] * q_refs[-1][...]
    dots = dots_of(image, q_refs)
    image, beta = orthogonal(image, dots, q_refs)
    last_ref[...] = image
    coef = put(put(c_ref[...], 0, k, dots[-1]), 1, k, beta)
    c_out[...] = coef[: c_out.shape[0], : c_out.shape[1]]
    groups = image.shape[0] // 3
    row = lax.axis_index(ROW)
    group = row // 2
    place = row % 2 * 2 + lax.axis_index("col")
    for j in range(3):
        for v, q in enumerate((*q_refs, last_ref)):
            piece_ref[8 * j + v : 8 * j + v + 1, :] = q[pl.ds(j * groups + group, 1), :]
    a, b, c = piece_ref[0:8, :], piece_ref[8:16, :], piece_ref[16:24, :]
    lane = lane_of(a.shape)
    one = jnp.where(lane < 32, pltpu.roll(a, 32, 1), pltpu.roll(b, 32, 1))
    two = jnp.where(lane < 64, pltpu.roll(b, 64, 1), pltpu.roll(c, 64, 1))
    three = pltpu.roll(c, 96, 1)
    out = jnp.where(place == 0, a, jnp.where(place == 1, one, jnp.where(place == 2, two, three)))
    newest = lax.broadcasted_iota(jnp.int32, out.shape, 0) == len(q_refs)
    out = out * jnp.float32(math.sqrt(full_dim)) * jnp.where(newest, 1.0 / beta, 1.0)
    basis_ref[...] = out[: basis_ref.shape[0], : basis_ref.shape[1]]


def call(body, outs, scratch, *args):
    vmem = pl.BlockSpec(memory_space=pltpu.VMEM)
    return pl.pallas_call(
        body,
        out_shape=[jax.ShapeDtypeStruct(s, jnp.float32) for s in outs],
        in_specs=[vmem] * len(args),
        out_specs=[vmem] * len(outs),
        scratch_shapes=[pltpu.VMEM(s, jnp.float32) for s in scratch],
        compiler_params=pltpu.CompilerParams(vmem_limit_bytes=16 << 20),
    )(*args)


def pair_call(pay, start, diagonal, matrix):
    hbm = pl.BlockSpec(memory_space=pltpu.HBM)
    cost = pl.CostEstimate(flops=0, transcendentals=0, bytes_accessed=4 * matrix.nbytes)
    return pl.pallas_call(
        pair_kernel,
        out_shape=jax.ShapeDtypeStruct(pay, jnp.float32),
        in_specs=[hbm] * 3,
        out_specs=pl.BlockSpec(memory_space=pltpu.VMEM),
        scratch_shapes=[
            pltpu.VMEM(start.shape, jnp.float32),
            pltpu.VMEM(diagonal.shape, jnp.float32),
            pltpu.VMEM((8, LANES), jnp.float32),
            pltpu.SemaphoreType.DMA((2,)),
        ],
        cost_estimate=cost,
        compiler_params=pltpu.CompilerParams(vmem_limit_bytes=16 << 20),
    )(*(pltpu.with_memory_space_constraint(x, pltpu.HBM) for x in (start, diagonal, matrix)))


def exchange(payload):
    return lax.all_to_all(payload, ORDER, 0, 0, tiled=True)


def local(matrix, diagonal, start):
    devices = lax.axis_size(ROW_COL)
    tile_len = start.shape[0]
    full_dim = tile_len * devices
    dense = (full_dim // LANES, LANES)
    pay = (2 * devices, LANES)
    payload = pair_call(pay, start.reshape(1, -1), diagonal.reshape(1, -1), matrix)
    gathered = exchange(payload)
    tile = (8, LANES)
    q, diag, part, payload = call(first_kernel, [dense, dense, tile, pay], [dense], gathered, matrix)
    basis, parts = [q], [part]
    coef = jnp.zeros(tile, jnp.float32)
    for k in range(ITERS - 1):
        gathered = exchange(payload)
        q, coef, payload, *part = call(
            functools.partial(middle_kernel, k),
            [dense, tile, pay] + [tile] * (k < ITERS - 2),
            [dense],
            *basis,
            *parts,
            diag,
            gathered,
            coef,
            matrix,
        )
        basis.append(q)
        parts += part
    gathered = exchange(payload)
    return tuple(
        call(
            functools.partial(last_kernel, ITERS - 1, full_dim),
            [(ITERS + 1, tile_len), (2, ITERS)],
            [dense, (24, LANES)],
            *basis,
            diag,
            gathered,
            coef,
        )
    )


def solution(mesh):
    split = Mesh(
        mesh.devices.reshape(4, 4, 4, mesh.shape["col"]), ("row_0", "row_1", "row_2", "col")
    )
    return jax.shard_map(
        local,
        mesh=split,
        in_specs=(P(ROW, "col"), P(ROW_COL), P(ROW_COL)),
        out_specs=(P(None, ROW_COL), P()),
        check_vma=False,
    )
```
